32 devices in a mesh: dp: 2 (over y), fsdp: 16 (over z, x, core).
Axes of the slice: x: 2, y: 2, z: 4, core: 2. Of those that a mesh axis runs over, the one named last changes fastest.
Arguments:
- queries: bfloat16 [6144, 2560], P(('dp', 'fsdp')), may hold values from -8 to 8
- keys: bfloat16 [6144, 2560], P(('dp', 'fsdp')), may hold values from -8 to 8
- values: bfloat16 [6144, 2560], P(('dp', 'fsdp')), may hold values from -6 to 6
- lengths: int32 [16, 2, 4], P('fsdp'), may hold values from 0 to 192, as said below
- normalized_weight: bfloat16 [2560, 5120], P(None, 'fsdp'), may hold values from -1 to 1
- block_scale_codes: int32 [40, 5120], P(None, 'fsdp'), may hold values from 0 to 255
- scale_group_factor: float32 [5, 5120], P(None, 'fsdp'), may hold values from 0.01 to 0.03
- scale_group_offset: float32 [5, 5120], P(None, 'fsdp'), may hold values from 0.005 to 0.015
- adapter_down_weight: bfloat16 [64, 2560], P(None, 'fsdp'), may hold values from -0.125 to 0.125
- adapter_up_weight: bfloat16 [64, 5120], P(None, 'fsdp'), may hold values from -0.75 to 0.75
- cotangent: bfloat16 [6144, 5120], P(('dp', 'fsdp')), may hold values from -6 to 6
Outputs:
- projection_output: bfloat16 [6144, 5120], P(('dp', 'fsdp'))
- attention_gradient: bfloat16 [6144, 2560], P(('dp', 'fsdp'))
- down_grad: float32 [64, 2560], P(None, 'fsdp')
- adapter_up_gradient: float32 [64, 5120], P(None, 'fsdp')
The draws below stay inside these ranges and needn't reach their ends.
Inputs may be any that keep to these rules, and one draw needn't show every extreme that they name: The 4 lengths of each block sum to 192; zero lengths, if any, come last; some block is a single document of 192 tokens.
All inputs are finite; a program needn't handle non-finite values.
Results may differ from the reference program's by a relative error of at most 0.0059.
Values may be sent and summed in bfloat16 or wider, within the bound.
A program may use at most 192 MiB of HBM per device.

```python
import math
import jax
import jax.numpy as jnp
from jax import lax

MODEL_WIDTH = 5120
HEADS = 20
HEAD_SIZE = 128
ADAPTER_RANK = 64
QBLOCK = 64
SCALE_GROUP = 8
DOCS = 4
TOK_DEV = 192
HEAD_FEATURES = 2560
TOKENS = 6144
N_DP = 2
N_FSDP = 16


def draw_queries(key, part):
    noise = jax.random.normal(jax.random.fold_in(key, 11), (TOKENS, HEADS, HEAD_SIZE), jnp.float32)
    result = jnp.clip(noise, -6.0, 6.0)
    return result.reshape(TOKENS, HEAD_FEATURES).astype(jnp.bfloat16)


def draw_keys(key, part):
    noise = jax.random.normal(jax.random.fold_in(key, 12), (TOKENS, HEADS, HEAD_SIZE), jnp.float32)
    result = jnp.clip(noise, -6.0, 6.0)
    return result.reshape(TOKENS, HEAD_FEATURES).astype(jnp.bfloat16)


def draw_lengths(key, part):
    blocks = N_FSDP * N_DP
    doc_count = jax.random.randint(jax.random.fold_in(key, 21), (blocks,), 1, DOCS + 1)
    single = jax.random.randint(jax.random.fold_in(key, 22), (), 0, blocks)
    doc_count = jnp.where(jnp.arange(blocks) == single, 1, doc_count)
    scores = jax.random.randint(jax.random.fold_in(key, 23), (blocks, TOK_DEV - 1), 0, 2 ** 20) * TOK_DEV + jnp.arange(1, TOK_DEV, dtype=jnp.int32)[None, :]
    order = jnp.argsort(scores, axis=-1)
    picks = order[:, :DOCS - 1].astype(jnp.int32) + 1
    usable = jnp.arange(DOCS - 1, dtype=jnp.int32)[None, :] < doc_count[:, None] - 1
    cuts = jnp.sort(jnp.where(usable, picks, TOK_DEV), axis=-1)
    edges = jnp.concatenate([jnp.zeros((blocks, 1), jnp.int32), cuts.astype(jnp.int32), jnp.full((blocks, 1), TOK_DEV, jnp.int32)], axis=1)
    doc_lengths = edges[:, 1:] - edges[:, :-1]
    return doc_lengths.reshape(N_FSDP, N_DP, DOCS).astype(jnp.int32)


def set_ends(values, stream_key, least, largest):
    dims = values.shape
    place = [jax.random.randint(jax.random.fold_in(stream_key, axis), (), 0, dims[axis]) for axis in range(len(dims))]
    values = values.at[tuple(place)].set(least)
    longest = dims.index(max(dims))
    place[longest] = (place[longest] + 1) % dims[longest]
    return values.at[tuple(place)].set(largest)


def strengthened(entries, key, source, target, shards_of, factor):
    owner, partner = [(jnp.arange(entries.shape[dim]) // (entries.shape[dim] // shards_of)).reshape([-1 if axis == dim else 1 for axis in range(entries.ndim)]) for dim in (source, target)]
    chosen = jax.random.permutation(key, shards_of)[partner]
    strong = (owner == chosen) | (owner == (partner + shards_of // 2) % shards_of)
    return jnp.where(strong, factor * entries, entries)


def shard_levels(key, shape, split, smallest, largest):
    level = 1.0
    for dim, blocks in split:
        heights = jax.random.uniform(jax.random.fold_in(jax.random.fold_in(key, 6), dim), (blocks,), jnp.float32, smallest / len(split), largest / len(split))
        level = level * jnp.repeat(jnp.exp(heights), shape[dim] // blocks).reshape((-1,) + (1,) * (len(shape) - 1 - dim))
    return level


def scatter_about(own_key, shape, deviation, bound, split=(), kind=jnp.bfloat16):
    level = shard_levels(own_key, shape, split, -0.22, 0.18) if split else 1.0
    drawn = jax.random.normal(own_key, shape, jnp.float32) * deviation * level
    return jnp.minimum(jnp.maximum(drawn, -bound), bound).astype(kind)


def bell_draw_with(rng, extent, width, most, cuts, heavy, kind=jnp.bfloat16):
    array = width * jax.random.normal(rng, extent, jnp.float32)
    if cuts:
        array = array * shard_levels(rng, extent, cuts, -0.22, 0.18)
    return jnp.clip(strengthened(array, jax.random.fold_in(rng, 3), *heavy), -most, most).astype(kind)


def setup_inputs(seed: int = 0) -> dict:
    key_list = jax.random.split(jax.random.key(seed), 12)
    return {
        "queries": draw_queries(jax.random.fold_in(key_list[11], 71), 0),
        "keys": draw_keys(jax.random.fold_in(key_list[11], 71), 0),
        "values": scatter_about(key_list[2], (TOKENS, HEAD_FEATURES), 1.0, 6.0, ((0, 32),)),
        "lengths": draw_lengths(jax.random.fold_in(key_list[11], 71), 0),
        "normalized_weight": jnp.clip(jax.random.uniform(key_list[4], (HEAD_FEATURES, MODEL_WIDTH), jnp.float32, -1.0, 1.0) * shard_levels(key_list[4], (HEAD_FEATURES, MODEL_WIDTH), ((1, 16),), -0.4, 0.0), -1.0, 1.0).astype(jnp.bfloat16),
        "block_scale_codes": set_ends(jax.random.randint(key_list[5], (HEAD_FEATURES // QBLOCK, MODEL_WIDTH), 0, 256), jax.random.fold_in(key_list[5], 1), 0, 255).astype(jnp.int32),
        "scale_group_factor": jnp.clip(jnp.exp(math.log(0.03) - 1.0986123 * jax.random.uniform(key_list[6], (HEAD_FEATURES // (QBLOCK * SCALE_GROUP), MODEL_WIDTH), jnp.float32) ** shard_levels(key_list[6], (HEAD_FEATURES // (QBLOCK * SCALE_GROUP), MODEL_WIDTH), ((1, 16),), -0.2, 0.2)), 0.01, 0.03),
        "scale_group_offset": jnp.clip(jnp.exp(math.log(0.015) - 1.0986123 * jax.random.uniform(key_list[7], (HEAD_FEATURES // (QBLOCK * SCALE_GROUP), MODEL_WIDTH), jnp.float32) ** shard_levels(key_list[7], (HEAD_FEATURES // (QBLOCK * SCALE_GROUP), MODEL_WIDTH), ((1, 16),), -0.2, 0.2)), 0.005, 0.015),
        "adapter_down_weight": scatter_about(key_list[8], (ADAPTER_RANK, HEAD_FEATURES), HEAD_FEATURES ** -0.5, 0.125, ((1, 16),)),
        "adapter_up_weight": scatter_about(key_list[9], (ADAPTER_RANK, MODEL_WIDTH), ADAPTER_RANK ** -0.5, 0.75, ((1, 16),)),
        "cotangent": bell_draw_with(key_list[10], (TOKENS, MODEL_WIDTH), 1.0, 6.0, ((0, 32),), (0, 1, 32, 2.75)),
    }


adapter_scale = 0.25


def dequantize(normalized_weight, block_scale_codes, scale_group_factor, scale_group_offset):
    spread_scale = jnp.repeat(scale_group_factor, SCALE_GROUP, axis=0)
    spread_offset = jnp.repeat(scale_group_offset, SCALE_GROUP, axis=0)
    absmax = spread_scale * (block_scale_codes.astype(jnp.float32) + 1.0) / 256.0 + spread_offset
    return (normalized_weight.astype(jnp.float32) * jnp.repeat(absmax, QBLOCK, axis=0)).astype(jnp.bfloat16)


def attend_block(operands):
    queries, keys, values, doc_lengths = operands
    doc_ends = jnp.cumsum(doc_lengths)
    places = jnp.arange(TOK_DEV, dtype=jnp.int32)
    segment = jnp.sum((doc_ends[None, :] <= places[:, None]).astype(jnp.int32), axis=1)
    allowed = (segment[:, None] == segment[None, :]) & (places[None, :] <= places[:, None])
    query_heads = queries.reshape(TOK_DEV, HEADS, HEAD_SIZE).astype(jnp.float32)
    key_heads = keys.reshape(TOK_DEV, HEADS, HEAD_SIZE).astype(jnp.float32)
    value_heads = values.reshape(TOK_DEV, HEADS, HEAD_SIZE).astype(jnp.float32)
    scores = jnp.einsum("qhe,khe->hqk", query_heads, key_heads) * (HEAD_SIZE ** -0.5)
    scores = jnp.where(allowed[None], scores, -jnp.inf)
    row_max = jnp.max(scores, axis=-1, keepdims=True)
    weights = jnp.exp(scores - row_max)
    total = jnp.sum(weights, axis=-1)
    rounded = lax.optimization_barrier(weights.astype(jnp.bfloat16)).astype(jnp.float32)
    mixed = jnp.einsum("hqk,khe->qhe", rounded, value_heads) / jnp.transpose(total)[:, :, None]
    return mixed.astype(jnp.bfloat16).reshape(TOK_DEV, HEAD_FEATURES)


def reference(queries, keys, values, lengths, normalized_weight, block_scale_codes, scale_group_factor, scale_group_offset, adapter_down_weight, adapter_up_weight, cotangent):
    blocks = N_DP * N_FSDP
    block_lengths = jnp.transpose(lengths, (1, 0, 2)).reshape(blocks, DOCS)
    attention_output = lax.map(attend_block, (queries.reshape(blocks, TOK_DEV, HEAD_FEATURES), keys.reshape(blocks, TOK_DEV, HEAD_FEATURES), values.reshape(blocks, TOK_DEV, HEAD_FEATURES), block_lengths))
    attention_output = attention_output.reshape(TOKENS, HEAD_FEATURES)
    frozen_output = dequantize(normalized_weight, block_scale_codes, scale_group_factor, scale_group_offset)
    reduced_activation = jnp.dot(attention_output, adapter_down_weight.T, preferred_element_type=jnp.float32).astype(jnp.bfloat16)
    projection_output = (jnp.dot(attention_output, frozen_output, preferred_element_type=jnp.float32) + adapter_scale * jnp.dot(reduced_activation, adapter_up_weight, preferred_element_type=jnp.float32)).astype(jnp.bfloat16)
    reduced_gradient = (adapter_scale * jnp.dot(cotangent, adapter_up_weight.T, preferred_element_type=jnp.float32)).astype(jnp.bfloat16)
    attention_gradient = (jnp.dot(cotangent, frozen_output.T, preferred_element_type=jnp.float32) + jnp.dot(reduced_gradient, adapter_down_weight, preferred_element_type=jnp.float32)).astype(jnp.bfloat16)
    down_grad = jnp.dot(reduced_gradient.T, attention_output, preferred_element_type=jnp.float32)
    adapter_up_gradient = adapter_scale * jnp.dot(reduced_activation.T, cotangent, preferred_element_type=jnp.float32)
    return projection_output, attention_gradient, down_grad, adapter_up_gradient
```

```python
import functools

import jax
import jax.numpy as jnp
from jax import lax
from jax.experimental import pallas as pl
from jax.experimental.pallas import tpu as pltpu
from jax.sharding import PartitionSpec as P

HEAD_SIZE = 128
QBLOCK = 64
SCALE_GROUP = 8


adapter_scale = 0.25


def dequantize(normalized_weight, block_scale_codes, scale_group_factor, scale_group_offset):
    spread_scale = jnp.repeat(scale_group_factor, SCALE_GROUP, axis=0)
    spread_offset = jnp.repeat(scale_group_offset, SCALE_GROUP, axis=0)
    absmax = spread_scale * (block_scale_codes.astype(jnp.float32) + 1.0) / 256.0 + spread_offset
    return (normalized_weight.astype(jnp.float32) * jnp.repeat(absmax, QBLOCK, axis=0)).astype(
        jnp.bfloat16
    )


def attend(queries, keys, values, doc_lengths):
    tokens = queries.shape[0]
    head_count = queries.shape[1] // HEAD_SIZE
    query_heads = queries.reshape(tokens, head_count, HEAD_SIZE)
    key_heads = keys.reshape(tokens, head_count, HEAD_SIZE)
    value_heads = values.reshape(tokens, head_count, HEAD_SIZE)
    doc_ends = jnp.cumsum(doc_lengths)
    places = jnp.arange(tokens, dtype=jnp.int32)
    segment = jnp.sum((doc_ends[None, :] <= places[:, None]).astype(jnp.int32), axis=1)
    allowed = (segment[:, None] == segment[None, :]) & (places[None, :] <= places[:, None])
    scores = jnp.einsum(
        "qhe,khe->hqk", query_heads, key_heads, preferred_element_type=jnp.float32
    ) * HEAD_SIZE ** (-0.5)
    scores = jnp.where(allowed[None], scores, -jnp.inf)
    row_max = jnp.max(scores, axis=-1, keepdims=True)
    weights = jnp.exp(scores - row_max)
    total = jnp.sum(weights, axis=-1)
    summed = jnp.einsum(
        "hqk,khe->qhe",
        weights.astype(jnp.bfloat16),
        value_heads,
        preferred_element_type=jnp.float32,
    )
    return (
        (summed / jnp.transpose(total)[:, :, None])
        .astype(jnp.bfloat16)
        .reshape(tokens, head_count * HEAD_SIZE)
    )


MESH = pl.DeviceIdType.MESH


def ring_kernel(scatter, third, *refs):
    if scatter:
        block, parts, out, mine, sems, ring_send, ring_recv, row_send, row_recv = refs[:9]
        core_send, core_recv, part_send, part_recv = refs[9:]
    else:
        block, out, sems, ring_send, ring_recv, row_send, row_recv, core_send, core_recv = refs
    n = lax.axis_size("fsdp")
    chips = n // 2
    half = chips // 2
    row = lax.axis_index("dp")
    me = lax.axis_index("fsdp")
    chip, core = me // 2, me % 2
    place = jnp.where(chip % 2 == 0, chip // 2, chips - 1 - chip // 2)

    def device_at(where):
        where = (where + chips) % chips
        there = jnp.where(where < half, 2 * where, 2 * (chips - 1 - where) + 1)
        return 2 * there + core

    neighbour = (device_at(place + 1), device_at(place - 1))
    twin = 2 * chip + 1 - core
    other_row = row + 1 - 2 * (row % 2)
    parity = row % 2
    size = block.shape[0]
    own = (pl.ds(pl.multiple_of(parity * third, 16), third))
    others = (pl.ds(pl.multiple_of((1 - parity) * third, 16), third))
    rest = pl.ds(2 * third, size - 2 * third)
    segments = (own, rest)

    barrier = pltpu.get_barrier_semaphore()
    if scatter:
        for k in range(1, n):
            pl.semaphore_signal(barrier, inc=1, device_id={"fsdp": (me + k) % n}, device_id_type=MESH)
        pl.semaphore_signal(barrier, inc=1, device_id={"dp": other_row}, device_id_type=MESH)
        pl.semaphore_wait(barrier, n)
    else:
        for peer in (*neighbour, twin):
            pl.semaphore_signal(barrier, inc=1, device_id={"fsdp": peer}, device_id_type=MESH)
        pl.semaphore_signal(barrier, inc=1, device_id={"dp": other_row}, device_id_type=MESH)
        pl.semaphore_wait(barrier, 4)

    sent = []

    def send(src, dst, send_sem, recv_sem, target):
        copy = pltpu.make_async_remote_copy(
            src_ref=src, dst_ref=dst, send_sem=send_sem, recv_sem=recv_sem,
            device_id=target, device_id_type=MESH,
        )
        copy.start()
        sent.append(copy)

    def arrived(dst, recv_sem, send_sem):
        pltpu.make_async_remote_copy(
            src_ref=dst, dst_ref=dst, send_sem=send_sem, recv_sem=recv_sem,
            device_id={"fsdp": twin}, device_id_type=MESH,
        ).wait_recv()

    hops = ((half, half - 1), (half - 1, half))

    def ring(src, origin, way, seg, step):
        send(
            src, out.at[origin, segments[seg]], ring_send.at[way, seg, step],
            ring_recv.at[way, seg, step], {"fsdp": neighbour[way]},
        )

    for seg in range(2):
        for way in range(2):
            if hops[way][seg] >= 1:
                ring(block.at[segments[seg]], me, way, seg, 0)
    send(block, out.at[me], core_send.at[0, 0, 2], core_recv.at[0, 0, 2], {"fsdp": twin})
    if scatter:
        for k in range(1, n):
            to = (me + k) % n
            send(parts.at[to], mine.at[me], part_send.at[k], part_recv.at[k], {"fsdp": to})
    keep = pltpu.make_async_copy(block, out.at[me], sems.at[0])
    keep.start()
    if scatter:
        keep_part = pltpu.make_async_copy(parts.at[me], mine.at[me], sems.at[1])
        keep_part.start()

    def origin_of(way, step):
        return device_at(place - step if way == 0 else place + step)

    def to_twin(origin, rows, way, step, kind):
        send(
            out.at[origin, rows], out.at[origin, rows], core_send.at[way, step, kind],
            core_recv.at[way, step, kind], {"fsdp": twin},
        )

    def from_row(way, step):
        origin = origin_of(way, step)
        arrived(out.at[origin, others], row_recv.at[way, step], row_send.at[way, step])
        to_twin(origin, others, way, step, 2)

    for step in range(1, half + 1):
        for seg in range(2):
            for way in range(2):
                if step <= hops[way][seg]:
                    origin = origin_of(way, step)
                    rows = segments[seg]
                    view = out.at[origin, rows]
                    arrived(view, ring_recv.at[way, seg, step - 1], ring_send.at[way, seg, step - 1])
                    if step < hops[way][seg]:
                        ring(view, origin, way, seg, step)
                    if seg == 0:
                        send(
                            view, view, row_send.at[way, step], row_recv.at[way, step],
                            {"dp": other_row},
                        )
                    to_twin(origin, rows, way, step, seg)
        for way in range(2):
            if 1 <= step - 1 <= hops[way][0]:
                from_row(way, step - 1)
    for way in range(2):
        if 1 <= half <= hops[way][0]:
            from_row(way, half)

    arrived(out.at[twin], core_recv.at[0, 0, 2], core_send.at[0, 0, 2])
    for way in range(2):
        for step in range(1, half + 1):
            there = origin_of(way, step)
            origin = there + 1 - 2 * core
            for seg in range(2):
                if step <= hops[way][seg]:
                    arrived(
                        out.at[origin, segments[seg]], core_recv.at[way, step, seg],
                        core_send.at[way, step, seg],
                    )
            if step <= hops[way][0]:
                arrived(out.at[origin, others], core_recv.at[way, step, 2], core_send.at[way, step, 2])
    if scatter:
        for k in range(1, n):
            arrived(mine.at[(me + n - k) % n], part_recv.at[k], part_send.at[k])
        keep_part.wait()
    keep.wait()
    for copy in sent:
        copy.wait_send()


def ring_gather(block, collective_id, parts=None):
    n = lax.axis_size("fsdp")
    half = n // 4
    rows, width = block.shape
    third = rows // 16 // 3 * 16
    scatter = parts is not None
    out_shape = [jax.ShapeDtypeStruct((n, rows, width), block.dtype)]
    any_spec = pl.BlockSpec(memory_space=pl.ANY)
    dma = pltpu.SemaphoreType.DMA
    scratch = [
        dma((2,)),
        dma((2, 2, half + 1)), dma((2, 2, half + 1)),
        dma((2, half + 1)), dma((2, half + 1)),
        dma((2, half + 1, 3)), dma((2, half + 1, 3)),
    ]
    operands = [block]
    if scatter:
        out_shape.append(jax.ShapeDtypeStruct(parts.shape, parts.dtype))
        scratch += [dma((n,)), dma((n,))]
        operands.append(parts)
    return pl.pallas_call(
        functools.partial(ring_kernel, scatter, third),
        out_shape=out_shape,
        in_specs=[pl.BlockSpec(memory_space=pltpu.VMEM)] * len(operands),
        out_specs=[any_spec] * len(out_shape),
        scratch_shapes=scratch,
        compiler_params=pltpu.CompilerParams(
            collective_id=collective_id, has_side_effects=True, vmem_limit_bytes=24 * 2**20
        ),
    )(*operands)


def per_device(
    queries,
    keys,
    values,
    lengths,
    normalized_weight,
    block_scale_codes,
    scale_group_factor,
    scale_group_offset,
    adapter_down_weight,
    adapter_up_weight,
    cotangent,
):
    n = lax.axis_size("fsdp")
    row_index = lax.axis_index("dp")
    rank, down_width = adapter_down_weight.shape
    up_width = adapter_up_weight.shape[1]
    own_rows = down_width + up_width
    packed_rows = own_rows * rank // 128
    padded_rows = -(-packed_rows // 16) * 16

    def pack(x):
        x = x.reshape(*x.shape[:-2], packed_rows, 128)
        pad = [(0, 0)] * (x.ndim - 2) + [(0, padded_rows - packed_rows), (0, 0)]
        return jnp.pad(x, pad)

    def unpack(x):
        return x[..., :packed_rows, :].reshape(*x.shape[:-2], own_rows, rank)

    own_lengths = lax.dynamic_index_in_dim(lengths[0], row_index, 0, keepdims=False)
    own_adapters = jnp.concatenate([adapter_up_weight.T, adapter_down_weight.T], axis=0)
    (adapters,) = ring_gather(pack(own_adapters), 0)
    adapters = unpack(adapters)
    up_rows = adapters[:, :up_width].reshape(n * up_width, rank)
    down_rows = adapters[:, up_width:].reshape(n * down_width, rank)

    attention_output = attend(queries, keys, values, own_lengths)
    reduced_activation = jnp.dot(
        attention_output, down_rows, preferred_element_type=jnp.float32
    ).astype(jnp.bfloat16)
    reduced_gradient = (
        adapter_scale * jnp.dot(cotangent, up_rows, preferred_element_type=jnp.float32)
    ).astype(jnp.bfloat16)
    down_part = jnp.dot(attention_output.T, reduced_gradient, preferred_element_type=jnp.float32)
    up_part = adapter_scale * jnp.dot(
        cotangent.T, reduced_activation, preferred_element_type=jnp.float32
    )
    parts = jnp.concatenate(
        [up_part.reshape(n, up_width, rank), down_part.reshape(n, down_width, rank)], axis=1
    ).astype(jnp.bfloat16)

    local_base = dequantize(
        normalized_weight, block_scale_codes, scale_group_factor, scale_group_offset
    )
    gathered, shares = ring_gather(local_base.T, 1, pack(parts))
    base_rows = gathered.reshape(-1, gathered.shape[2])
    share = lax.psum(jnp.sum(shares.astype(jnp.float32), axis=0), "dp")
    share = unpack(share)

    product = lax.dot_general(
        attention_output, base_rows, (((1,), (1,)), ((), ())), preferred_element_type=jnp.float32
    )
    projection_output = (
        product
        + adapter_scale
        * lax.dot_general(
            reduced_activation, up_rows, (((1,), (1,)), ((), ())),
            preferred_element_type=jnp.float32,
        )
    ).astype(jnp.bfloat16)
    attention_gradient = (
        jnp.dot(cotangent, base_rows, preferred_element_type=jnp.float32)
        + lax.dot_general(
            reduced_gradient, down_rows, (((1,), (1,)), ((), ())),
            preferred_element_type=jnp.float32,
        )
    ).astype(jnp.bfloat16)
    return (projection_output, attention_gradient, share[up_width:].T, share[:up_width].T)


def solution(mesh):
    return jax.shard_map(
        per_device,
        mesh=mesh,
        in_specs=(
            P(("dp", "fsdp"), None),
            P(("dp", "fsdp"), None),
            P(("dp", "fsdp"), None),
            P("fsdp", None, None),
            P(None, "fsdp"),
            P(None, "fsdp"),
            P(None, "fsdp"),
            P(None, "fsdp"),
            P(None, "fsdp"),
            P(None, "fsdp"),
            P(("dp", "fsdp"), None),
        ),
        out_specs=(
            P(("dp", "fsdp"), None),
            P(("dp", "fsdp"), None),
            P(None, "fsdp"),
            P(None, "fsdp"),
        ),
        check_vma=False,
    )
```

```python
import functools

import jax
import jax.numpy as jnp
from jax import lax
from jax.experimental import pallas as pl
from jax.experimental.pallas import tpu as pltpu
from jax.sharding import PartitionSpec as P

HEAD_SIZE = 128
QBLOCK = 64
SCALE_GROUP = 8


adapter_scale = 0.25


def dequantize_kernel(weight, absmax, out):
    rows, features = out.shape
    lane = lax.broadcasted_iota(jnp.int32, (rows, 2 * QBLOCK), 1)
    for i in range(features // (2 * QBLOCK)):
        columns = slice(2 * QBLOCK * i, 2 * QBLOCK * (i + 1))
        scale = jnp.where(
            lane < QBLOCK, absmax[:, 2 * i : 2 * i + 1], absmax[:, 2 * i + 1 : 2 * i + 2]
        )
        out[:, columns] = (weight[:, columns].astype(jnp.float32) * scale).astype(out.dtype)


def dequantize(normalized_weight, block_scale_codes, scale_group_factor, scale_group_offset):
    spread_scale = jnp.repeat(scale_group_factor, SCALE_GROUP, axis=0)
    spread_offset = jnp.repeat(scale_group_offset, SCALE_GROUP, axis=0)
    absmax = spread_scale * (block_scale_codes.astype(jnp.float32) + 1.0) / 256.0 + spread_offset
    weight = normalized_weight.T
    return pl.pallas_call(
        dequantize_kernel,
        out_shape=jax.ShapeDtypeStruct(weight.shape, jnp.bfloat16),
        compiler_params=pltpu.CompilerParams(vmem_limit_bytes=16 * 2**20),
    )(weight, absmax.T)


def attend(queries, keys, values, doc_lengths):
    tokens = queries.shape[0]
    head_count = queries.shape[1] // HEAD_SIZE
    query_heads = queries.reshape(tokens, head_count, HEAD_SIZE)
    key_heads = keys.reshape(tokens, head_count, HEAD_SIZE)
    value_heads = values.reshape(tokens, head_count, HEAD_SIZE)
    doc_ends = jnp.cumsum(doc_lengths)
    places = jnp.arange(tokens, dtype=jnp.int32)
    segment = jnp.sum((doc_ends[None, :] <= places[:, None]).astype(jnp.int32), axis=1)
    allowed = (segment[:, None] == segment[None, :]) & (places[None, :] <= places[:, None])
    scores = jnp.einsum(
        "qhe,khe->hqk", query_heads, key_heads, preferred_element_type=jnp.float32
    ) * HEAD_SIZE ** (-0.5)
    scores = jnp.where(allowed[None], scores, -jnp.inf)
    row_max = jnp.max(scores, axis=-1, keepdims=True)
    weights = jnp.exp(scores - row_max)
    total = jnp.sum(weights, axis=-1)
    summed = jnp.einsum(
        "hqk,khe->qhe",
        weights.astype(jnp.bfloat16),
        value_heads,
        preferred_element_type=jnp.float32,
    )
    return (
        (summed / jnp.transpose(total)[:, :, None])
        .astype(jnp.bfloat16)
        .reshape(tokens, head_count * HEAD_SIZE)
    )


MESH = pl.DeviceIdType.MESH


def ring_kernel(scatter, third, *refs):
    if scatter:
        block, parts, out, mine, sems, ring_send, ring_recv, row_send, row_recv = refs[:9]
        core_send, core_recv, part_send, part_recv = refs[9:]
    else:
        block, out, sems, ring_send, ring_recv, row_send, row_recv, core_send, core_recv = refs
    n = lax.axis_size("fsdp")
    chips = n // 2
    half = chips // 2
    row = lax.axis_index("dp")
    me = lax.axis_index("fsdp")
    chip, core = me // 2, me % 2
    place = jnp.where(chip % 2 == 0, chip // 2, chips - 1 - chip // 2)

    def device_at(where):
        where = (where + chips) % chips
        there = jnp.where(where < half, 2 * where, 2 * (chips - 1 - where) + 1)
        return 2 * there + core

    neighbour = (device_at(place + 1), device_at(place - 1))
    twin = 2 * chip + 1 - core
    other_row = row + 1 - 2 * (row % 2)
    parity = row % 2
    size = block.shape[0]
    own = (pl.ds(pl.multiple_of(parity * third, 16), third))
    others = (pl.ds(pl.multiple_of((1 - parity) * third, 16), third))
    rest = pl.ds(2 * third, size - 2 * third)
    segments = (own, rest)

    barrier = pltpu.get_barrier_semaphore()
    if scatter:
        for k in range(1, n):
            pl.semaphore_signal(barrier, inc=1, device_id={"fsdp": (me + k) % n}, device_id_type=MESH)
        pl.semaphore_signal(barrier, inc=1, device_id={"dp": other_row}, device_id_type=MESH)
        pl.semaphore_wait(barrier, n)
    else:
        for peer in (*neighbour, twin):
            pl.semaphore_signal(barrier, inc=1, device_id={"fsdp": peer}, device_id_type=MESH)
        pl.semaphore_signal(barrier, inc=1, device_id={"dp": other_row}, device_id_type=MESH)
        pl.semaphore_wait(barrier, 4)

    sent = []

    def send(src, dst, send_sem, recv_sem, target):
        copy = pltpu.make_async_remote_copy(
            src_ref=src, dst_ref=dst, send_sem=send_sem, recv_sem=recv_sem,
            device_id=target, device_id_type=MESH,
        )
        copy.start()
        sent.append(copy)

    def arrived(dst, recv_sem, send_sem):
        pltpu.make_async_remote_copy(
            src_ref=dst, dst_ref=dst, send_sem=send_sem, recv_sem=recv_sem,
            device_id={"fsdp": twin}, device_id_type=MESH,
        ).wait_recv()

    hops = ((half, half - 1), (half - 1, half))

    def ring(src, origin, way, seg, step):
        send(
            src, out.at[origin, segments[seg]], ring_send.at[way, seg, step],
            ring_recv.at[way, seg, step], {"fsdp": neighbour[way]},
        )

    for seg in range(2):
        for way in range(2):
            if hops[way][seg] >= 1:
                ring(block.at[segments[seg]], me, way, seg, 0)
    send(block, out.at[me], core_send.at[0, 0, 2], core_recv.at[0, 0, 2], {"fsdp": twin})
    if scatter:
        for k in range(1, n):
            to = (me + k) % n
            send(parts.at[to], mine.at[me], part_send.at[k], part_recv.at[k], {"fsdp": to})
    keep = pltpu.make_async_copy(block, out.at[me], sems.at[0])
    keep.start()
    if scatter:
        keep_part = pltpu.make_async_copy(parts.at[me], mine.at[me], sems.at[1])
        keep_part.start()

    def origin_of(way, step):
        return device_at(place - step if way == 0 else place + step)

    def to_twin(origin, rows, way, step, kind):
        send(
            out.at[origin, rows], out.at[origin, rows], core_send.at[way, step, kind],
            core_recv.at[way, step, kind], {"fsdp": twin},
        )

    def from_row(way, step):
        origin = origin_of(way, step)
        arrived(out.at[origin, others], row_recv.at[way, step], row_send.at[way, step])
        to_twin(origin, others, way, step, 2)

    for step in range(1, half + 1):
        for seg in range(2):
            for way in range(2):
                if step <= hops[way][seg]:
                    origin = origin_of(way, step)
                    rows = segments[seg]
                    view = out.at[origin, rows]
                    arrived(view, ring_recv.at[way, seg, step - 1], ring_send.at[way, seg, step - 1])
                    if step < hops[way][seg]:
                        ring(view, origin, way, seg, step)
                    if seg == 0:
                        send(
                            view, view, row_send.at[way, step], row_recv.at[way, step],
                            {"dp": other_row},
                        )
                    to_twin(origin, rows, way, step, seg)
        for way in range(2):
            if 1 <= step - 1 <= hops[way][0]:
                from_row(way, step - 1)
    for way in range(2):
        if 1 <= half <= hops[way][0]:
            from_row(way, half)

    arrived(out.at[twin], core_recv.at[0, 0, 2], core_send.at[0, 0, 2])
    for way in range(2):
        for step in range(1, half + 1):
            there = origin_of(way, step)
            origin = there + 1 - 2 * core
            for seg in range(2):
                if step <= hops[way][seg]:
                    arrived(
                        out.at[origin, segments[seg]], core_recv.at[way, step, seg],
                        core_send.at[way, step, seg],
                    )
            if step <= hops[way][0]:
                arrived(out.at[origin, others], core_recv.at[way, step, 2], core_send.at[way, step, 2])
    if scatter:
        for k in range(1, n):
            arrived(mine.at[(me + n - k) % n], part_recv.at[k], part_send.at[k])
        keep_part.wait()
    keep.wait()
    for copy in sent:
        copy.wait_send()


def ring_gather(block, collective_id, parts=None):
    n = lax.axis_size("fsdp")
    half = n // 4
    rows, width = block.shape
    third = (rows // 16 + 2) // 3 * 16
    scatter = parts is not None
    out_shape = [jax.ShapeDtypeStruct((n, rows, width), block.dtype)]
    any_spec = pl.BlockSpec(memory_space=pl.ANY)
    dma = pltpu.SemaphoreType.DMA
    scratch = [
        dma((2,)),
        dma((2, 2, half + 1)), dma((2, 2, half + 1)),
        dma((2, half + 1)), dma((2, half + 1)),
        dma((2, half + 1, 3)), dma((2, half + 1, 3)),
    ]
    operands = [block]
    if scatter:
        out_shape.append(jax.ShapeDtypeStruct(parts.shape, parts.dtype))
        scratch += [dma((n,)), dma((n,))]
        operands.append(parts)
    return pl.pallas_call(
        functools.partial(ring_kernel, scatter, third),
        out_shape=out_shape,
        in_specs=[pl.BlockSpec(memory_space=pltpu.VMEM)] * len(operands),
        out_specs=[any_spec] * len(out_shape),
        scratch_shapes=scratch,
        compiler_params=pltpu.CompilerParams(
            collective_id=collective_id, has_side_effects=True, vmem_limit_bytes=24 * 2**20
        ),
    )(*operands)


def row_sum_kernel(rows, share, out, landed, send_sems, recv_sems):
    me = lax.axis_index("dp")
    barrier = pltpu.get_barrier_semaphore()
    for k in range(1, rows):
        pl.semaphore_signal(barrier, inc=1, device_id={"dp": (me + k) % rows}, device_id_type=MESH)
    pl.semaphore_wait(barrier, rows - 1)
    copies = []
    for k in range(1, rows):
        copy = pltpu.make_async_remote_copy(
            src_ref=share, dst_ref=landed.at[me], send_sem=send_sems.at[k],
            recv_sem=recv_sems.at[k], device_id={"dp": (me + k) % rows}, device_id_type=MESH,
        )
        copy.start()
        copies.append(copy)
    keep = pltpu.make_async_copy(share, landed.at[me], send_sems.at[0])
    keep.start()
    for k in range(1, rows):
        pltpu.make_async_remote_copy(
            src_ref=share, dst_ref=landed.at[(me + rows - k) % rows], send_sem=send_sems.at[k],
            recv_sem=recv_sems.at[k], device_id={"dp": (me + k) % rows}, device_id_type=MESH,
        ).wait_recv()
    keep.wait()
    for copy in copies:
        copy.wait_send()
    total = landed[0]
    for k in range(1, rows):
        total = total + landed[k]
    out[...] = total


def sum_over_rows(share):
    rows = lax.axis_size("dp")
    vmem = pl.BlockSpec(memory_space=pltpu.VMEM)
    return pl.pallas_call(
        functools.partial(row_sum_kernel, rows),
        out_shape=jax.ShapeDtypeStruct(share.shape, share.dtype),
        in_specs=[vmem],
        out_specs=vmem,
        scratch_shapes=[
            pltpu.VMEM((rows, *share.shape), share.dtype),
            pltpu.SemaphoreType.DMA((rows,)),
            pltpu.SemaphoreType.DMA((rows,)),
        ],
        compiler_params=pltpu.CompilerParams(
            collective_id=2, has_side_effects=True, vmem_limit_bytes=16 * 2**20
        ),
    )(share)


def per_device(
    queries,
    keys,
    values,
    lengths,
    normalized_weight,
    block_scale_codes,
    scale_group_factor,
    scale_group_offset,
    adapter_down_weight,
    adapter_up_weight,
    cotangent,
):
    n = lax.axis_size("fsdp")
    row_index = lax.axis_index("dp")
    rank, down_width = adapter_down_weight.shape
    up_width = adapter_up_weight.shape[1]
    own_rows = down_width + up_width
    packed_rows = own_rows * rank // 128
    padded_rows = -(-packed_rows // 16) * 16

    def pack(x):
        x = x.reshape(*x.shape[:-2], packed_rows, 128)
        pad = [(0, 0)] * (x.ndim - 2) + [(0, padded_rows - packed_rows), (0, 0)]
        return jnp.pad(x, pad)

    def unpack(x):
        return x[..., :packed_rows, :].reshape(*x.shape[:-2], own_rows, rank)

    own_lengths = lax.dynamic_index_in_dim(lengths[0], row_index, 0, keepdims=False)
    own_adapters = jnp.concatenate([adapter_up_weight.T, adapter_down_weight.T], axis=0)
    (adapters,) = ring_gather(pack(own_adapters), 0)
    adapters = unpack(adapters)
    up_rows = adapters[:, :up_width].reshape(n * up_width, rank)
    down_rows = adapters[:, up_width:].reshape(n * down_width, rank)

    attention_output = attend(queries, keys, values, own_lengths)
    reduced_activation = jnp.dot(
        attention_output, down_rows, preferred_element_type=jnp.float32
    ).astype(jnp.bfloat16)
    reduced_gradient = (
        adapter_scale * jnp.dot(cotangent, up_rows, preferred_element_type=jnp.float32)
    ).astype(jnp.bfloat16)
    down_part = jnp.dot(attention_output.T, reduced_gradient, preferred_element_type=jnp.float32)
    up_part = adapter_scale * jnp.dot(
        cotangent.T, reduced_activation, preferred_element_type=jnp.float32
    )
    parts = jnp.concatenate(
        [up_part.reshape(n, up_width, rank), down_part.reshape(n, down_width, rank)], axis=1
    ).astype(jnp.bfloat16)

    local_base = dequantize(
        normalized_weight, block_scale_codes, scale_group_factor, scale_group_offset
    )
    gathered, shares = ring_gather(local_base, 1, pack(parts))
    base_rows = gathered.reshape(-1, gathered.shape[2])
    share = unpack(sum_over_rows(jnp.sum(shares.astype(jnp.float32), axis=0)))

    product = lax.dot_general(
        attention_output, base_rows, (((1,), (1,)), ((), ())), preferred_element_type=jnp.float32
    )
    projection_output = (
        product
        + adapter_scale
        * lax.dot_general(
            reduced_activation, up_rows, (((1,), (1,)), ((), ())),
            preferred_element_type=jnp.float32,
        )
    ).astype(jnp.bfloat16)
    attention_gradient = (
        jnp.dot(cotangent, base_rows, preferred_element_type=jnp.float32)
        + lax.dot_general(
            reduced_gradient, down_rows, (((1,), (1,)), ((), ())),
            preferred_element_type=jnp.float32,
        )
    ).astype(jnp.bfloat16)
    return (projection_output, attention_gradient, share[up_width:].T, share[:up_width].T)


def solution(mesh):
    return jax.shard_map(
        per_device,
        mesh=mesh,
        in_specs=(
            P(("dp", "fsdp"), None),
            P(("dp", "fsdp"), None),
            P(("dp", "fsdp"), None),
            P("fsdp", None, None),
            P(None, "fsdp"),
            P(None, "fsdp"),
            P(None, "fsdp"),
            P(None, "fsdp"),
            P(None, "fsdp"),
            P(None, "fsdp"),
            P(("dp", "fsdp"), None),
        ),
        out_specs=(
            P(("dp", "fsdp"), None),
            P(("dp", "fsdp"), None),
            P(None, "fsdp"),
            P(None, "fsdp"),
        ),
        check_vma=False,
    )
```
